512 devices in a mesh: doc: 8 (over x, core), seq: 64 (over z, y).
Axes of the slice: x: 4, y: 4, z: 16, core: 2. Of those that a mesh axis runs over, the one named last changes fastest.
Arguments:
- queries: bfloat16 [65536, 1792], P(('doc', 'seq')), parts along dimension 0, may hold values from -5 to 5
- keys: bfloat16 [65536, 256], P(('doc', 'seq')), parts along dimension 0, may hold values from -5 to 5
- values: bfloat16 [65536, 256], P(('doc', 'seq')), parts along dimension 0, may hold values from -6 to 6
- doc_length: int32 [8], P('doc'), parts along dimension 0, may hold values from 4096 to 8192
- sink_pos: int32 [32], P('doc'), parts along dimension 0, may hold values from 0 to 127, as said below
Outputs:
- attended: bfloat16 [65536, 1792], P(('doc', 'seq')), parts along dimension 0
- row_lse: float32 [14, 65536], P(None, ('doc', 'seq')), parts along dimension 1
- sink_mass: float32 [14, 65536], P(None, ('doc', 'seq')), parts along dimension 1
- head_lse: float32 [112], P('doc'), parts along dimension 0
- head_sink: float32 [112], P('doc'), parts along dimension 0
The draws below stay inside these ranges and needn't reach their ends.
There are 8 independent parts, one for each index of `doc`. The reference program is written for one: setup_inputs(seed, part) draws one part's arguments, and reference() takes and returns one part's arrays. A program takes and returns all parts, laid end to end along the dimension named above; each array names one. Nothing has to cross between parts.
Inputs may be any that keep to these rules, and one draw needn't show every extreme that they name: `sink_pos`: 4 distinct positions within the document's first 128 tokens; positions 0 and 127 are always among them. Positions from doc_length up to 8192 are padding.
All inputs are finite; a program needn't handle non-finite values.
Results may differ from the reference program's by a relative error of at most 0.009.
Values may be sent and summed in bfloat16 or wider, within the bound.
No kernel may reach another device: no remote copies, remote signals or barrier semaphores. Data moves between devices by JAX's collectives and lax.ppermute only.
A program may use at most 64 MiB of HBM per device.

```python
import jax
import jax.numpy as jnp
from jax import lax

QUERY_HEADS = 14
KEY_VALUE_HEADS = 2
HEAD_DIMENSION = 128
NSINK = 4
S_DEV = 128
PADDED_LENGTH = 8192


def draw_queries(key, part):
    query_group_width = QUERY_HEADS // KEY_VALUE_HEADS
    unsharded_result = jnp.clip(jax.random.normal(jax.random.fold_in(key, 11), (PADDED_LENGTH, KEY_VALUE_HEADS, query_group_width, HEAD_DIMENSION), jnp.float32), -5.0, 5.0)
    return unsharded_result.reshape(PADDED_LENGTH, QUERY_HEADS * HEAD_DIMENSION).astype(jnp.bfloat16)


def draw_keys(key, part):
    unsharded_result = jnp.clip(jax.random.normal(jax.random.fold_in(key, 13), (PADDED_LENGTH, KEY_VALUE_HEADS, HEAD_DIMENSION), jnp.float32), -5.0, 5.0)
    return unsharded_result.reshape(PADDED_LENGTH, KEY_VALUE_HEADS * HEAD_DIMENSION).astype(jnp.bfloat16)


def draw_sink_pos(key, part):
    order = jax.random.permutation(jax.random.fold_in(key, 17), S_DEV - 2)
    middle = order[:NSINK - 2].astype(jnp.int32) + 1
    first = jnp.zeros((1,), jnp.int32)
    last = jnp.full((1,), S_DEV - 1, jnp.int32)
    return jnp.concatenate([first, middle, last]).astype(jnp.int32)


def level_of(key, extent, split, low, top_value):
    loudness, own = 1.0, jax.random.fold_in(key, 6)
    for dim, shards_of in split:
        draws = jnp.exp(jax.random.uniform(jax.random.fold_in(own, dim), (shards_of,), jnp.float32, low / len(split), top_value / len(split)))
        loudness = loudness * jnp.repeat(draws, extent[dim] // shards_of).reshape([-1 if axis == dim else 1 for axis in range(len(extent))])
    return loudness


def scatter_about(rng, extent, deviation, most, pieces=(), kind=jnp.bfloat16):
    drawn = jax.random.normal(rng, extent, jnp.float32) * deviation
    if len(pieces) > 0:
        drawn = level_of(rng, extent, pieces, -0.22, 0.18) * drawn
    return jnp.clip(drawn, min=-most, max=most).astype(kind)


def setup_inputs(seed: int = 0, part: int = 0) -> dict:
    splits = jax.random.split(jax.random.key(seed), 6)
    own_keys = jax.random.split(jax.random.fold_in(splits[5], part), 6)
    return {
        "queries": draw_queries(jax.random.fold_in(jax.random.fold_in(splits[5], part), 71), part),
        "keys": draw_keys(jax.random.fold_in(jax.random.fold_in(splits[5], part), 71), part),
        "values": scatter_about(own_keys[2], (PADDED_LENGTH, KEY_VALUE_HEADS * HEAD_DIMENSION), 1.0, 6.0, ((0, 64),)),
        "doc_length": jax.random.randint(own_keys[3], (1,), PADDED_LENGTH // 2, PADDED_LENGTH + 1).astype(jnp.int32),
        "sink_pos": draw_sink_pos(jax.random.fold_in(jax.random.fold_in(splits[5], part), 71), part),
    }


def reference(queries, keys, values, doc_length, sink_pos):
    query_group_width = QUERY_HEADS // KEY_VALUE_HEADS
    length = doc_length[0]
    key_float = keys.reshape(PADDED_LENGTH, KEY_VALUE_HEADS, HEAD_DIMENSION).astype(jnp.float32)
    value_float = values.reshape(PADDED_LENGTH, KEY_VALUE_HEADS, HEAD_DIMENSION).astype(jnp.float32)
    key_pos = jnp.arange(PADDED_LENGTH, dtype=jnp.int32)
    is_sink = jnp.any(key_pos[:, None] == sink_pos[None, :], axis=1)
    rows_per_block = min(512, PADDED_LENGTH)
    block_count = PADDED_LENGTH // rows_per_block
    score_scale = HEAD_DIMENSION ** -0.5

    def one_block(block_index):
        first = (block_index * rows_per_block).astype(jnp.int32)
        query_float = lax.dynamic_slice_in_dim(queries, first, rows_per_block, 0)
        query_float = query_float.reshape(rows_per_block, KEY_VALUE_HEADS, query_group_width, HEAD_DIMENSION).astype(jnp.float32)
        scores = jnp.einsum("sgcd,pgd->gcsp", query_float, key_float, precision=lax.Precision.HIGHEST) * score_scale
        query_pos = first + jnp.arange(rows_per_block, dtype=jnp.int32)
        allowed = (key_pos[None, :] <= query_pos[:, None]) & (key_pos[None, :] < length)
        masked = jnp.where(allowed, scores, -jnp.inf)
        peak = jnp.max(masked, axis=-1, keepdims=True)
        row_lse = peak[..., 0] + jnp.log(jnp.sum(jnp.exp(masked - peak), axis=-1))
        probs = jnp.exp(masked - row_lse[..., None])
        sink_mass = jnp.sum(jnp.where(is_sink, probs, 0.0), axis=-1)
        rounded = lax.optimization_barrier(probs.astype(jnp.bfloat16)).astype(jnp.float32)
        attended = jnp.einsum("gcsp,pgd->sgcd", rounded, value_float, precision=lax.Precision.HIGHEST)
        attended = attended.reshape(rows_per_block, QUERY_HEADS * HEAD_DIMENSION)
        live_rows = query_pos < length
        attended = jnp.where(live_rows[:, None], attended, 0.0).astype(jnp.bfloat16)
        row_lse = jnp.where(live_rows[None, :], row_lse.reshape(QUERY_HEADS, rows_per_block), 0.0)
        sink_mass = jnp.where(live_rows[None, :], sink_mass.reshape(QUERY_HEADS, rows_per_block), 0.0)
        return attended, row_lse, sink_mass

    attended, row_lse, sink_mass = lax.map(one_block, jnp.arange(block_count, dtype=jnp.int32))
    attended = attended.reshape(PADDED_LENGTH, QUERY_HEADS * HEAD_DIMENSION)
    row_lse = row_lse.transpose(1, 0, 2).reshape(QUERY_HEADS, PADDED_LENGTH)
    sink_mass = sink_mass.transpose(1, 0, 2).reshape(QUERY_HEADS, PADDED_LENGTH)
    doc_count = length.astype(jnp.float32)
    head_lse = jnp.sum(row_lse, axis=1) / doc_count
    head_sink = jnp.sum(sink_mass, axis=1) / doc_count
    return (attended, row_lse, sink_mass, head_lse, head_sink)
```

```python
import functools
import math

import jax
import jax.numpy as jnp
from jax import lax
from jax.experimental import pallas as pl
from jax.experimental.pallas import tpu as pltpu
from jax.sharding import Mesh, PartitionSpec as P

C2 = math.log2(math.e) / math.sqrt(128.0)
LN2 = math.log(2.0)
NEG = -1e30
NZ = 16
def flash_kernel(RT, CH, info_ref, sink_ref, q_ref, *refs):
    blocks = refs[:NZ]
    o_ref, st_ref, k_s, v_s, m_s, acc_s = refs[NZ:]
    h = pl.program_id(0)
    z = info_ref[0]; live = info_ref[1]; half = info_ref[2]
    @pl.when((h == 0) & (live > 0))
    def _():
        ones = jnp.ones((256, 128), jnp.bfloat16)
        for t in range(NZ):
            k_s[t*256:(t+1)*256, :] = blocks[t][:, :128]
            v_s[t*256:(t+1)*256, :128] = blocks[t][:, 128:]
            v_s[t*256:(t+1)*256, 128:] = ones
    def chunk(start, size, masked, first):
        for r in range(512 // RT):
            rows = slice(r*RT, (r+1)*RT)
            s = lax.dot_general(q_ref[rows, :], k_s[pl.ds(start, size), :], (((1,), (1,)), ((), ())), preferred_element_type=jnp.float32)
            if masked:
                ri = lax.broadcasted_iota(jnp.int32, (RT, size), 0) + r*RT
                ci = lax.broadcasted_iota(jnp.int32, (RT, size), 1)
                ok = jnp.where(ci < 256, ci + half*256, jnp.where(z > 0, 0, 4096)) <= ri
                s = jnp.where(ok, s, NEG)
            mx = jnp.max(s, axis=1, keepdims=True)
            if first:
                m_new = mx
            else:
                m_old = m_s[rows, :1]
                m_new = jnp.maximum(m_old, mx)
                alpha = jnp.exp2((m_old - m_new) * C2)
            p = jnp.exp2((s - m_new) * C2)
            if masked:
                p = jnp.where(ok, p, 0.0)
            pv = jnp.dot(p.astype(jnp.bfloat16), v_s[pl.ds(start, size), :], preferred_element_type=jnp.float32)
            if first:
                acc_s[rows, :] = pv
            else:
                acc_s[rows, :] = acc_s[rows, :] * alpha + pv
            m_s[rows, :] = jnp.broadcast_to(m_new, (RT, 128))
    @pl.when(live > 0)
    def _():
        chunk(0, 512, True, True)
        nb = CH // 256
        nfull = jnp.maximum(z - 1, 0) // nb
        def step(c, _):
            chunk(pl.multiple_of(512 + c*CH, 256), CH, False, False)
            return 0
        lax.fori_loop(0, nfull, step, 0)
        done = nfull * nb + 2
        def tail(c, _):
            chunk(pl.multiple_of((done + c)*256, 256), 256, False, False)
            return 0
        lax.fori_loop(0, jnp.maximum(z + 1 - done, 0), tail, 0)
        l = acc_s[:, 128:]
        some = l > 0.0
        inv = 1.0 / jnp.where(some, l, 1.0)
        o_ref[...] = (acc_s[:, :128] * inv).astype(jnp.bfloat16)
        lse2 = jnp.where(some, m_s[...] * C2 + jnp.log2(jnp.where(some, l, 1.0)), NEG)
        s = lax.dot_general(q_ref[...], k_s[pl.ds(pl.multiple_of(z*256, 256), 128), :], (((1,), (1,)), ((), ())), preferred_element_type=jnp.float32)
        ri = lax.broadcasted_iota(jnp.int32, (512, 128), 0)
        ci = lax.broadcasted_iota(jnp.int32, (512, 128), 1)
        ok = jnp.where(z > 0, 0, ci) + sink_ref[...] <= ri
        pm = jnp.where(ok, jnp.exp2(jnp.where(ok, s * C2 - lse2, 0.0)), 0.0)
        sk = jnp.sum(pm, axis=1, keepdims=True)
        st_ref[0, 0:1, :] = (lse2 * LN2).T[0:1, :]
        st_ref[0, 1:2, :] = jnp.broadcast_to(sk, (512, 128)).T[0:1, :]
    @pl.when(live == 0)
    def _():
        o_ref[...] = jnp.zeros_like(o_ref)
        st_ref[...] = jnp.zeros_like(st_ref)
def flash(info, sink, q, blocks, RT=256, CH=512):
    n = len(blocks)
    return pl.pallas_call(
        functools.partial(flash_kernel, RT, CH),
        out_shape=(jax.ShapeDtypeStruct((512, 896), jnp.bfloat16), jax.ShapeDtypeStruct((7, 2, 512), jnp.float32)),
        grid_spec=pltpu.PrefetchScalarGridSpec(
            num_scalar_prefetch=1, grid=(7,),
            in_specs=[pl.BlockSpec((1, 128), lambda h, i: (0, 0)),
                      pl.BlockSpec((512, 128), lambda h, i: (0, h))]
                     + [pl.BlockSpec((256, 256), lambda h, i: (0, 0))] * n,
            out_specs=(pl.BlockSpec((512, 128), lambda h, i: (0, h)), pl.BlockSpec((1, 2, 512), lambda h, i: (h, 0, 0))),
            scratch_shapes=[pltpu.VMEM((4096, 128), jnp.bfloat16), pltpu.VMEM((4096, 256), jnp.bfloat16),
                            pltpu.VMEM((512, 128), jnp.float32), pltpu.VMEM((512, 256), jnp.float32)]),
        compiler_params=pltpu.CompilerParams(dimension_semantics=("arbitrary",), vmem_limit_bytes=48*1024*1024),
        cost_estimate=pl.CostEstimate(flops=2*3584*4096*128*2, bytes_accessed=4*1024*1024, transcendentals=3584*4096),
    )(info, sink, q, *blocks)


def shifted(value, axis, pairs):
    return lax.ppermute(value, axis, pairs)


def body(queries, keys, values, doc_length, sink_pos):
    z = lax.axis_index("z")
    y = lax.axis_index("y")
    group = y % 2
    half = y // 2
    length = doc_length[0]
    row_first = (z * 4 + y) * 128
    kv0 = jnp.concatenate([keys[:, :128], values[:, :128]], axis=1)
    kv1 = jnp.concatenate([keys[:, 128:], values[:, 128:]], axis=1)
    even = group == 0
    mine = jnp.where(even, kv0, kv1)
    other = jnp.where(even, kv1, kv0)
    got = lax.ppermute(other, "y", [(0, 1), (1, 0), (2, 3), (3, 2)])
    own = jnp.concatenate([jnp.where(even, mine, got), jnp.where(even, got, mine)], axis=0)

    by_group = jnp.stack([queries[:, :896], queries[:, 896:]] * 2)
    shared = lax.all_to_all(by_group, "y", 0, 0, tiled=True).reshape(512, 896)

    blocks = [None] * 16
    blocks[0] = own
    up, down = own, own
    for t in range(1, 9):
        up = lax.ppermute(up, "z", [(s, s + 1) for s in range(t - 1, 15)])
        blocks[t] = up
        if t < 8:
            down = lax.ppermute(down, "z", sorted(((b - t + 1) % 16, (b - t) % 16) for b in range(7)))
            blocks[16 - t] = down

    is_sink = jnp.any(jnp.arange(128, dtype=jnp.int32)[None, :] == sink_pos[:, None], axis=0)
    far = jnp.where(is_sink & (half == 0), 0, 4096).astype(jnp.int32)[None, :]
    live = (z * 512 < length).astype(jnp.int32)
    info = jnp.stack([z, live, half]).astype(jnp.int32)
    partial, stats = flash(info, far, shared, blocks, RT=256, CH=1024)

    stats = stats.reshape(7, 2, 4, 128).transpose(2, 0, 1, 3).reshape(4, 14, 128)
    stats = lax.all_to_all(stats, "y", 0, 0, tiled=True).reshape(2, 2, 7, 2, 128)
    parts = lax.all_to_all(partial.reshape(4, 128, 896), "y", 0, 0, tiled=True)

    lse = stats[:, :, :, 0, :]
    top = jnp.max(lse, axis=0)
    weight = jnp.exp(lse - top[None])
    total = jnp.sum(weight, axis=0)
    share = weight / total[None]
    live_rows = row_first + jnp.arange(128, dtype=jnp.int32) < length
    row_lse = jnp.where(live_rows[None, :], (top + jnp.log(total)).reshape(14, 128), 0.0)
    sink_mass = jnp.sum(share * stats[:, :, :, 1, :], axis=0).reshape(14, 128)
    sink_mass = jnp.where(live_rows[None, :], sink_mass, 0.0)

    sums = jnp.concatenate([jnp.sum(row_lse, axis=1), jnp.sum(sink_mass, axis=1)])
    everyone = lax.all_to_all(
        jnp.broadcast_to(sums[None], (64, 28)), ("z", "y"), 0, 0, tiled=True
    )
    totals = jnp.sum(everyone, axis=0) / length.astype(jnp.float32)

    share = jnp.where(live_rows, share, 0.0).reshape(2, 14, 128).transpose(0, 2, 1)
    parts = parts.reshape(2, 2, 128, 7, 128).astype(jnp.float32).transpose(0, 2, 1, 3, 4)
    parts = parts.reshape(2, 128, 14, 128)
    attended = jnp.sum(parts * share[..., None], axis=0).reshape(128, 1792).astype(jnp.bfloat16)
    return attended, row_lse, sink_mass, totals[:14], totals[14:]


def solution(mesh):
    plane = Mesh(mesh.devices.reshape(8, 16, 4), ("doc", "z", "y"))
    rows = ("doc", "z", "y")
    placed = (P(rows, None), P(rows, None), P(rows, None), P("doc"), P("doc"))
    return jax.shard_map(
        body,
        mesh=plane,
        in_specs=placed,
        out_specs=(P(rows, None), P(None, rows), P(None, rows), P("doc"), P("doc")),
        check_vma=False,
    )
```

```python
import functools
import math

import jax
import jax.numpy as jnp
import numpy as np
from jax import lax
from jax.experimental import pallas as pl
from jax.experimental.pallas import tpu as pltpu
from jax.sharding import Mesh, PartitionSpec as P


C2 = math.log2(math.e) / math.sqrt(128.0)
LN2 = math.log(2.0)
NEG = -1e30
RT = 256
HEADS = 7
MEETS = (2, 4, 6)
VM = pl.BlockSpec(memory_space=pltpu.VMEM)
SM = pl.BlockSpec(memory_space=pltpu.SMEM)
STATE = (
    jax.ShapeDtypeStruct((HEADS, 512, 128), jnp.float32),
    jax.ShapeDtypeStruct((HEADS, 512, 256), jnp.float32),
    jax.ShapeDtypeStruct((128, 128), jnp.bfloat16),
)


def transposed_dot(a, b):
    return lax.dot_general(a, b, (((1,), (1,)), ((), ())), preferred_element_type=jnp.float32)


def fold_in(q_ref, kv_ref, keys, m_ref, acc_ref, half=0, first=False, compact=False):
    kb = kv_ref[keys, :128]
    va = kv_ref[keys, 128:]
    va = jnp.concatenate([va, jnp.ones(va.shape, jnp.bfloat16)], axis=1)
    chains = [(h, slice(r, r + RT)) for h in range(HEADS) for r in range(0, 512, RT)]

    def scored(chain):
        h, rows = chain
        return transposed_dot(q_ref[rows, h * 128 : (h + 1) * 128], kb)

    def weighed(chain, s):
        h, rows = chain
        if first:
            ri = lax.broadcasted_iota(jnp.int32, (RT, 256), 0) + rows.start
            ci = lax.broadcasted_iota(jnp.int32, (RT, 256), 1) + half * 256
            ok = ci <= ri
            s = jnp.where(ok, s, NEG)
        top = jnp.broadcast_to(jnp.max(s, axis=1, keepdims=True), (RT, 128))
        alpha = None
        if not first:
            old = m_ref[h, rows, :]
            top = jnp.maximum(old, top)
            alpha = jnp.exp2((old - top) * C2)
        m_ref[h, rows, :] = top
        p = [jnp.exp2((s[:, i : i + 128] - top) * C2) for i in range(0, s.shape[1], 128)]
        p = jnp.concatenate(p, axis=1)
        if first:
            p = jnp.where(ok, p, 0.0)
        return p.astype(jnp.bfloat16), alpha

    def summed(chain, p, alpha):
        h, rows = chain
        o = jnp.dot(p, va, preferred_element_type=jnp.float32)
        if first:
            acc_ref[h, rows, :] = o
        else:
            acc_ref[h, rows, :128] = acc_ref[h, rows, :128] * alpha + o[:, :128]
            acc_ref[h, rows, 128:] = acc_ref[h, rows, 128:] * alpha + o[:, 128:]

    if compact:
        def one(h, _):
            cols = pl.ds(pl.multiple_of(h * 128, 128), 128)
            s = transposed_dot(q_ref[:, cols], kb)
            old = m_ref[h]
            top = jnp.maximum(old, jnp.broadcast_to(jnp.max(s, axis=1, keepdims=True), (512, 128)))
            alpha = jnp.exp2((old - top) * C2)
            m_ref[h] = top
            p = [jnp.exp2((s[:, i : i + 128] - top) * C2) for i in range(0, s.shape[1], 128)]
            o = jnp.dot(jnp.concatenate(p, axis=1).astype(jnp.bfloat16), va, preferred_element_type=jnp.float32)
            acc_ref[h, :, :128] = acc_ref[h, :, :128] * alpha + o[:, :128]
            acc_ref[h, :, 128:] = acc_ref[h, :, 128:] * alpha + o[:, 128:]
            return 0

        lax.fori_loop(0, HEADS, one, 0)
        return
    s = scored(chains[0])
    waiting = None
    for i, chain in enumerate(chains):
        ahead = scored(chains[i + 1]) if i + 1 < len(chains) else None
        if waiting is not None:
            summed(*waiting)
        waiting = (chain, *weighed(chain, s))
        s = ahead
    summed(*waiting)


def first_kernel(info_ref, q_ref, kv_ref, pair_ref, m_ref, acc_ref, sink_ref):
    @pl.when(info_ref[1] > 0)
    def _():
        fold_in(q_ref, kv_ref, slice(0, 256), m_ref, acc_ref, info_ref[2], True)
        sink = pl.ds(pl.multiple_of(info_ref[5] * 256, 256), 128)
        sink_ref[...] = pair_ref[sink, :128]

    @pl.when((info_ref[1] > 0) & (info_ref[6] > 0))
    def _():
        keys = pl.ds(pl.multiple_of((info_ref[6] - 1) * 256, 256), 256)
        fold_in(q_ref, pair_ref, keys, m_ref, acc_ref)


def next_kernel(i, info_ref, q_ref, pair_ref, m_in, acc_in, sink_in, m_ref, acc_ref, sink_ref):
    code = jnp.where(info_ref[1] > 0, info_ref[5 + i], 0)

    @pl.when(code == 2)
    def _():
        fold_in(q_ref, pair_ref, slice(0, 512), m_ref, acc_ref)

    @pl.when(code == 1)
    def _():
        fold_in(q_ref, pair_ref, slice(256, 512), m_ref, acc_ref, compact=True)

    @pl.when(info_ref[13 + i] > 0)
    def _():
        sink = pl.ds(pl.multiple_of(info_ref[5] * 256, 256), 128)
        sink_ref[...] = pair_ref[sink, :128]


def output_half_kernel(info_ref, acc_ref, st_ref, *o_refs):
    y = info_ref[4]

    @pl.when(info_ref[1] > 0)
    def _():
        for k, o_ref in enumerate(o_refs):
            rows = pl.ds(pl.multiple_of((y ^ k) * 128, 128), 128)
            for h in range(HEADS):
                total = acc_ref[h, rows, 128:]
                total = jnp.where(total > 0.0, total, 1.0)
                o_ref[:, h * 128 : (h + 1) * 128] = (acc_ref[h, rows, :128] * (1.0 / total)).astype(jnp.bfloat16)

    @pl.when(info_ref[1] == 0)
    def _():
        for o_ref in o_refs:
            o_ref[...] = jnp.zeros_like(o_ref)


def closing_kernel(info_ref, far_ref, q_ref, m_ref, acc_ref, sink_ref, met_ref, st_ref):
    @pl.when(info_ref[1] > 0)
    def _():
        lane = lax.broadcasted_iota(jnp.int32, (512, 128), 1)
        ri = lax.broadcasted_iota(jnp.int32, (512, 128), 0)
        hit = lane == far_ref[0]
        for i in range(1, 4):
            hit = jnp.logical_or(hit, lane == far_ref[i])
        reach = jnp.where(info_ref[0] > 0, 0, lane) + 4096 * info_ref[2]
        ok = jnp.where(hit, reach, 4096) <= ri
        table = jnp.zeros((512, 128), jnp.float32)
        keys = sink_ref[...]
        for h in range(HEADS):
            cols = slice(h * 128, (h + 1) * 128)
            total = acc_ref[h, :, 128:]
            some = total > 0.0
            total = jnp.where(some, total, 1.0)
            lse2 = jnp.where(some, m_ref[h] * C2 + jnp.log2(total), NEG)
            s = transposed_dot(q_ref[:, cols], keys)
            part = jnp.where(ok, jnp.exp2(jnp.where(ok, s * C2 - lse2, 0.0)), 0.0)
            mass = jnp.broadcast_to(jnp.sum(part, axis=1, keepdims=True), (512, 128))
            table = jnp.where(lane == h, lse2 * LN2, table)
            table = jnp.where(lane == 8 + h, mass, table)
        st_ref[...] = table.T[:16]

    @pl.when(info_ref[1] == 0)
    def _():
        st_ref[...] = jnp.zeros_like(st_ref)


def settle_kernel(info_ref, st_ref, lse_ref, mass_ref, share_ref, send_ref):
    z, length, y = info_ref[0], info_ref[3], info_ref[4]
    mine = pl.ds(pl.multiple_of(y * 128, 128), 128)

    def merged(a, b):
        top = jnp.maximum(a[:8], b[:8])
        wa = jnp.exp(a[:8] - top)
        wb = jnp.exp(b[:8] - top)
        both = wa + wb
        wa, wb = wa / both, wb / both
        return top + jnp.log(both), wa * a[8:] + wb * b[8:], wa, wb

    pos = z * 512 + lax.broadcasted_iota(jnp.int32, (8, 512), 1)
    own = z * 512 + y * 128 + lax.broadcasted_iota(jnp.int32, (8, 128), 1)
    shares, sums = [None] * 4, []
    for g in range(2):
        lse, mass, _, _ = merged(st_ref[g], st_ref[g + 2])
        for x in (lse, mass):
            x = jnp.sum(jnp.where(pos < length, x, 0.0), axis=1, keepdims=True)
            sums.append(jnp.broadcast_to(x, (8, 128)))
        lse, mass, wa, wb = merged(st_ref[g, :, mine], st_ref[g + 2, :, mine])
        lse_ref[g * 7 : g * 7 + 7, :] = jnp.where(own < length, lse, 0.0)[:7]
        mass_ref[g * 7 : g * 7 + 7, :] = jnp.where(own < length, mass, 0.0)[:7]
        shares[g] = jnp.where(own < length, wa, 0.0)
        shares[g + 2] = jnp.where(own < length, wb, 0.0)
    turned = []
    for k in range(4):
        turned.append(sum(jnp.where((y ^ k) == i, shares[i], 0.0) for i in range(4)))
    table = jnp.concatenate(turned + sums + [jnp.zeros((64, 128), jnp.float32)], axis=0).T
    share_ref[...] = table
    send_ref[...] = table[:16]


def output_kernel(info_ref, share_ref, *refs):
    parts, o_ref = refs[:4], refs[4]
    y = info_ref[4]
    for k in range(2):
        first = ((y + k) & 1) * 896
        for h in range(HEADS):
            cols = slice(h * 128, (h + 1) * 128)
            a = share_ref[:, k * 8 + h : k * 8 + h + 1]
            b = share_ref[:, (k + 2) * 8 + h : (k + 2) * 8 + h + 1]
            both = parts[k][:, cols].astype(jnp.float32) * a + parts[k + 2][:, cols].astype(jnp.float32) * b
            o_ref[:, pl.ds(pl.multiple_of(first + h * 128, 128), 128)] = both.astype(jnp.bfloat16)


def call(kernel, shapes, operands, flops, aliases=None, smem=1):
    return pl.pallas_call(
        kernel,
        out_shape=shapes,
        in_specs=[SM] * smem + [VM] * (len(operands) - smem),
        out_specs=jax.tree.map(lambda _: VM, shapes),
        input_output_aliases=aliases or {},
        compiler_params=pltpu.CompilerParams(vmem_limit_bytes=8 * 1024 * 1024),
        cost_estimate=pl.CostEstimate(flops=flops, bytes_accessed=1 << 20, transcendentals=flops // 512),
    )(*operands)


def position(z, turn):
    return (z + turn) % 16


def plan():
    rows = np.zeros((2, 16, 24), np.int32)
    for turn in range(2):
        for z in range(16):
            w = position(z, turn)
            rows[turn, z, 0] = 1 + (w ^ 1) % 2 if (((w ^ 1) - turn) % 16) < z else 0
            for i in range(2, 9):
                away = -(i // 2) if (i + w) % 2 == 0 else i // 2
                pair = (w // 2 + away) % 8
                early = [(2 * pair + k - turn) % 16 < z for k in range(2)]
                rows[turn, z, i - 1] = {(False, False): 0, (False, True): 1, (True, True): 2}[tuple(early)]
                rows[turn, z, i + 7] = pair == 0
    return rows


def hops(i):
    def beside(w, step):
        return (w + 1 if (w + step) % 2 else w - 1) % 16

    def needed(w, step, turn):
        if step == 1 or rows[turn, (w - turn) % 16, step - 1] > 0:
            return True
        return step < 8 and needed(beside(w, step + 1), step + 1, turn)

    rows = plan()
    pairs = []
    for doc in range(8):
        turn = doc % 2
        for w in range(16):
            to = beside(w, i)
            if needed(to, i, turn):
                pairs.append((doc * 16 + (w - turn) % 16, doc * 16 + (to - turn) % 16))
    return pairs


def exchange(value, axis):
    return lax.all_to_all(value, axis, 0, 0, tiled=True)


def attention(queries, keys, values, doc_length, sink_pos):
    z = lax.axis_index("z")
    y = lax.axis_index("y")
    half = y // 2
    length = doc_length[0]
    kv0 = jnp.concatenate([keys[:, :128], values[:, :128]], axis=1)
    kv1 = jnp.concatenate([keys[:, 128:], values[:, 128:]], axis=1)
    even = y % 2 == 0
    mine = jnp.where(even, kv0, kv1)
    other = jnp.where(even, kv1, kv0)
    got = lax.ppermute(other, "y", [(0, 1), (1, 0), (2, 3), (3, 2)])
    own = jnp.concatenate([jnp.where(even, mine, got), jnp.where(even, got, mine)], axis=0)

    by_group = jnp.stack([queries[:, :896], queries[:, 896:]] * 2)
    live = z * 512 < length
    turn = lax.axis_index("doc") % 2
    info = jnp.stack([z, live.astype(jnp.int32), half, length, y, turn]).astype(jnp.int32)
    info = jnp.concatenate([info, lax.dynamic_slice(jnp.asarray(plan()), (turn, z, 0), (1, 1, 24))[0, 0]])

    def swapped(value, i):
        return lax.ppermute(value, ("doc", "z"), hops(i))

    beside = swapped(own, 1)
    shared = exchange(by_group, "y").reshape(512, 896)
    low = position(z, turn) % 2 == 0
    pair = jnp.concatenate([jnp.where(low, own, beside), jnp.where(low, beside, own)], axis=0)
    moving = swapped(pair, 2)

    def folded(state, came, i):
        return call(
            functools.partial(next_kernel, i), STATE, (info, shared, came, *state),
            2 * 2 * 3584 * 256 * 256, {3 + k: k for k in range(3)},
        )

    met = jnp.zeros((8, 128), jnp.float32)
    state = ()
    before = None
    for i in range(2, 9):
        if i == MEETS[0]:
            met, info = lax.optimization_barrier((met, info))
        if i in MEETS:
            met = lax.ppermute(met, "doc", [(d, d ^ 1) for d in range(8)])
        came, met, *state = lax.optimization_barrier((moving, met, *state))
        if i < 8:
            moving = swapped(came, i + 1)
        if i == 2:
            state = call(first_kernel, STATE, (info, shared, own, pair), 3 * 3584 * 256 * 256)
        elif i == 3:
            state = folded(state, before, 2)
        else:
            if i == 4:
                state = folded(state, before, 3)
            state = folded(state, came, i)
        before = came

    stats = call(
        closing_kernel, jax.ShapeDtypeStruct((16, 512), jnp.float32), (info, sink_pos, shared, *state, met),
        3584 * 256 * 256, smem=2,
    )
    quarter = jax.ShapeDtypeStruct((128, 896), jnp.bfloat16)
    parts = list(call(output_half_kernel, (quarter,) * 4, (info, state[1], stats), 1 << 20))
    stats, *parts = lax.optimization_barrier((stats, *parts))
    everyone = exchange(jnp.broadcast_to(stats[None], (4, 16, 512)), "y")
    for k in range(1, 4):
        parts[k] = lax.ppermute(parts[k], "y", [(s, s ^ k) for s in range(4)])
    rows = jax.ShapeDtypeStruct((14, 128), jnp.float32)
    row_lse, sink_mass, share, send = call(
        settle_kernel,
        (rows, rows, jax.ShapeDtypeStruct((128, 128), jnp.float32), jax.ShapeDtypeStruct((16, 128), jnp.float32)),
        (info, everyone), 1 << 20,
    )
    sums = exchange(send, "z")
    totals = jnp.sum(sums, axis=0)[32:64].reshape(2, 2, 8)[:, :, :7] / length.astype(jnp.float32)
    attended = call(
        output_kernel, jax.ShapeDtypeStruct((128, 1792), jnp.bfloat16), (info, share, *parts), 1 << 20
    )
    return attended, row_lse, sink_mass, totals[:, 0].reshape(14), totals[:, 1].reshape(14)


def solution(mesh):
    plane = Mesh(mesh.devices.reshape(8, 16, 4), ("doc", "z", "y"))
    rows = ("doc", "z", "y")
    placed = (P(rows, None), P(rows, None), P(rows, None), P("doc"), P("doc"))
    return jax.shard_map(
        attention,
        mesh=plane,
        in_specs=placed,
        out_specs=(P(rows, None), P(None, rows), P(None, rows), P("doc"), P("doc")),
        check_vma=False,
    )
```
